32 devices in a mesh: dp: 8 (over z, x), mp: 4 (over y, core).
Axes of the slice: x: 2, y: 2, z: 4, core: 2. Of those that a mesh axis runs over, the one named last changes fastest.
Arguments:
- sparse_vecs: bfloat16 [8192, 26, 128], P(('dp', 'mp')), may hold values from -6 to 6
- dense_vec: bfloat16 [8192, 128], P(('dp', 'mp')), may hold values from -6 to 6
- top_cot: bfloat16 [8192, 1024], P(('dp', 'mp')), may hold values from -0.59765625 to 0.59765625
- top_weight: bfloat16 [479, 1024], replicated, may hold values from -0.25 to 0.25
- owner_ids: int32 [8192, 26, 1], P(('dp', 'mp')), may hold values from 0 to 7; in each aligned block of 6656 rows (0 to 6655, 6656 to 13311, ..., all dimensions but the last counted through in order) at most 1664 rows name the same one
- local_rows: int32 [8192, 26], P(('dp', 'mp')), may hold values from 0 to 127
- table: float32 [26, 1024, 128], P(None, ('dp', 'mp')), may hold values from -0.6 to 0.6
- accum: float32 [26, 1024], P(None, ('dp', 'mp')), may hold values from 0.05 to 2
Outputs:
- dense_grad: bfloat16 [8192, 128], P(('dp', 'mp'))
- new_table: float32 [26, 1024, 128], P(None, ('dp', 'mp'))
- new_accum: float32 [26, 1024], P(None, ('dp', 'mp'))
The draws below stay inside these ranges and needn't reach their ends.
Inputs may be any that keep to these rules, and one draw needn't show every extreme that they name: `owner_ids`: among the lookups of one device's 256 samples no owner group is named more than 1664 times; in every draw some device names some owner group exactly 1664 times.
All inputs are finite; a program needn't handle non-finite values.
Results may differ from the reference program's by a relative error of at most 0.005.
Values may be sent and summed in bfloat16 or wider, within the bound.
A program may use at most 128 MiB of HBM per device.

```python
import math
import jax
import jax.numpy as jnp
import numpy as np
from jax import lax

E = 128
TABLES = 26
H1 = 1024
B_DEV = 256
ZIN = 479
BATCH = 8192
LOOK_DEV = 6656
ROWS_GRP = 128
ROWS = 1024
CAP = 1664
N_DP = 8


def with_ends(drawn, rng, low, high):
    place = [jax.random.randint(jax.random.fold_in(rng, axis), (), 0, length) for axis, length in enumerate(drawn.shape)]
    main_axis = drawn.shape.index(max(drawn.shape))
    next_to = place[:main_axis] + [(place[main_axis] + 1) % drawn.shape[main_axis]] + place[main_axis + 1:]
    return drawn.at[tuple(place)].set(low).at[tuple(next_to)].set(high)


def shard_levels(key, extent, pieces, low, largest):
    def one(axis_at, shards_of):
        steps = jax.random.uniform(jax.random.fold_in(jax.random.fold_in(key, 6), axis_at), (shards_of,), jnp.float32, low / len(pieces), largest / len(pieces))
        return jnp.repeat(jnp.exp(steps), extent[axis_at] // shards_of).reshape((-1,) + (1,) * (len(extent) - axis_at - 1))

    gain = one(*pieces[0])
    for cut in pieces[1:]:
        gain = gain * one(*cut)
    return gain


def rank_bounds(count, lean):
    loads = [(1 << 20) // math.isqrt(standing ** lean) + 1 for standing in range(1, count + 1)]
    spread = 1 + sum(loads) // (1 << 30)
    return np.cumsum(np.array([max(1, weight // spread) for weight in loads]))


def ranked(key, dims, amount, lean):
    listing = rank_bounds(amount, lean)
    ticket = jax.random.randint(jax.random.fold_in(key, 1), dims, 0, int(listing[amount - 1]))
    standing = jnp.searchsorted(jnp.asarray(listing, jnp.int32), ticket, side="right")
    return jax.random.permutation(jax.random.fold_in(key, 2), amount)[standing].astype(jnp.int32)


def shared_out(own_key, own, number, rows, number_of, top, most, slope):
    order = jax.random.permutation(own_key, number_of)
    heavy_load, usual = load_shares(number_of, rows * top, most, slope, True), load_shares(number_of, rows * top, most, slope, False)
    places = jnp.arange(number_of)

    def named(sizes, rotation):
        used = int((sizes > 0).sum())
        fixed = max(1, used // 4)
        moved = fixed + (places - fixed + rotation * (used - fixed)) % max(1, number_of - fixed)
        return jnp.zeros((number_of,), jnp.int32).at[order[jnp.where(places < fixed, places, moved)]].set(jnp.asarray(sizes, jnp.int32))

    sizes = jnp.where(number % 4 == 0, named(heavy_load, number // 4), named(usual, number - number // 4 - 1))
    mixed = jax.random.permutation(jax.random.fold_in(own, 3), number_of)
    donor, taker = mixed[0:number_of // 2 * 2:2], mixed[1:number_of // 2 * 2:2]
    room = jnp.minimum(sizes[donor] - 1, most - sizes[taker]) // 2
    room = jnp.where((donor == order[0]) | (taker == order[0]) | (sizes[taker] == 0), 0, jnp.maximum(room, 0))
    moved = jax.random.randint(jax.random.fold_in(own, 4), (number_of // 2,), 0, 1 << 20) % (room + 1)
    sizes = sizes.at[donor].add(-moved).at[taker].add(moved)
    members = jnp.searchsorted(jnp.cumsum(sizes), jnp.arange(rows * top), side="right").astype(jnp.int32)
    table = members.reshape(top, rows).T
    table = table[jax.random.permutation(jax.random.fold_in(own, 1), rows)]
    rotation = jax.random.randint(jax.random.fold_in(own, 2), (rows, 1), 0, top)
    return jnp.take_along_axis(table, (jnp.arange(top)[None, :] + rotation) % top, axis=1)


def load_shares(amount, total, most, lean, full):
    loads = [(1 << 20) // math.isqrt(grade ** lean) + 1 for grade in range(1, amount + 1)]
    largest = most if full else min(most, max(-(-total // amount), total * loads[0] // sum(loads)))
    least = 1 if total - largest >= amount - 1 else 0
    counts, surplus = [largest] + [least] * (amount - 1), total - largest - least * (amount - 1)
    while surplus > 0:
        free = [i for i in range(1, amount) if counts[i] < largest] or [i for i in range(1, amount) if counts[i] < most]
        pool, budget = sum([loads[i] for i in free]), surplus
        for i in free:
            more = min(most - counts[i], max(1, budget * loads[i] // pool), surplus)
            counts[i] = counts[i] + more
            surplus = surplus - more
    return np.array(counts)


def scatter_about(key, dims, scale, most, shards=(), kind=jnp.bfloat16):
    level = shard_levels(key, dims, shards, -0.22, 0.18) if shards else 1.0
    array = jax.random.normal(key, dims, jnp.float32) * scale * level
    return jnp.minimum(jnp.maximum(array, -most), most).astype(kind)


def setup_inputs(seed: int = 0) -> dict:
    seeds = jax.random.split(jax.random.key(seed), 9)
    sparse_vecs = scatter_about(seeds[0], (BATCH, TABLES, E), 1.0, 6.0, ((0, 32),))
    dense_vec = scatter_about(seeds[1], (BATCH, E), 1.0, 6.0, ((0, 32),))
    top_cot = scatter_about(seeds[2], (BATCH, H1), 0.1, 0.59765625, ((0, 32),))
    top_weight = scatter_about(seeds[3], (ZIN, H1), ZIN ** -0.5, 0.25)
    owner_ids_keys = jax.random.split(jax.random.fold_in(seeds[4], 1), BATCH * TABLES // LOOK_DEV)
    owner_ids_turns = jax.random.permutation(jax.random.fold_in(seeds[4], 3), BATCH * TABLES // LOOK_DEV)
    owner_ids = jax.vmap(lambda own, number: shared_out(jax.random.fold_in(seeds[4], 2), own, number, LOOK_DEV, N_DP, 1, CAP, 1))(owner_ids_keys, owner_ids_turns).reshape((BATCH, TABLES, 1))
    local_rows = with_ends(ranked(seeds[5], (BATCH, TABLES), ROWS_GRP, 2), jax.random.fold_in(seeds[5], 3), 0, ROWS_GRP - 1).astype(jnp.int32)
    table = scatter_about(seeds[6], (TABLES, ROWS, E), 0.1, 0.6, ((1, 32),), jnp.float32)
    accum = jnp.clip(jnp.exp(math.log(2.0) - 3.6888794 * jax.random.uniform(seeds[7], (TABLES, ROWS), jnp.float32) ** shard_levels(seeds[7], (TABLES, ROWS), ((1, 32),), -0.2, 0.2)), 0.05, 2.0)
    return dict(sparse_vecs=sparse_vecs, dense_vec=dense_vec, top_cot=top_cot, top_weight=top_weight, owner_ids=owner_ids, local_rows=local_rows, table=table, accum=accum)


LEARN_RATE = 0.1
EPSILON = 1e-08

def pair_matrix(feature_count):
    row_index, col_index = np.tril_indices(feature_count, -1)
    pair_count = row_index.shape[0]
    matrix = np.zeros((pair_count, feature_count * feature_count), np.float32)
    matrix[np.arange(pair_count), row_index * feature_count + col_index] = 1.0
    matrix[np.arange(pair_count), col_index * feature_count + row_index] = 1.0
    return matrix

def interaction(sparse_vecs, dense_vec, top_cot, top_weight):
    batch_rows, table_count, row_width = sparse_vecs.shape
    feature_count = table_count + 1
    input_cot = jnp.dot(top_cot, top_weight.T, preferred_element_type=jnp.float32)
    symmetric = jnp.dot(input_cot[:, row_width:], pair_matrix(feature_count), precision=lax.Precision.HIGHEST)
    symmetric = symmetric.reshape(batch_rows, feature_count, feature_count)
    features = jnp.concatenate([dense_vec[:, None, :], sparse_vecs], axis=1).astype(jnp.float32)
    feature_grad = jnp.einsum('bij,bje->bie', symmetric, features, precision=lax.Precision.HIGHEST)
    dense_grad = (input_cot[:, :row_width] + feature_grad[:, 0]).astype(jnp.bfloat16)
    sparse_grad = feature_grad[:, 1:].astype(jnp.bfloat16)
    return (dense_grad, sparse_grad)

def reference(sparse_vecs, dense_vec, top_cot, top_weight, owner_ids, local_rows, table, accum):
    block_count = BATCH // B_DEV

    def one_block(blocks):
        return interaction(blocks[0], blocks[1], blocks[2], top_weight)
    dense_grad, sparse_grad = lax.map(one_block, (sparse_vecs.reshape(block_count, B_DEV, TABLES, E), dense_vec.reshape(block_count, B_DEV, E), top_cot.reshape(block_count, B_DEV, H1)))
    dense_grad = dense_grad.reshape(BATCH, E)
    sparse_grad = sparse_grad.reshape(BATCH, TABLES, E)
    row_total = ROWS_GRP * N_DP
    row_keys = jnp.arange(TABLES, dtype=jnp.int32)[None, :] * row_total + owner_ids[:, :, 0] * ROWS_GRP + local_rows
    row_grad = jax.ops.segment_sum(sparse_grad.astype(jnp.float32).reshape(BATCH * TABLES, E), row_keys.reshape(BATCH * TABLES).astype(jnp.int32), num_segments=TABLES * row_total)
    row_grad = row_grad.reshape(TABLES, row_total, E)
    new_accum = accum + lax.optimization_barrier(jnp.mean(row_grad * row_grad, axis=-1))
    new_table = table - LEARN_RATE * row_grad / (jnp.sqrt(new_accum)[:, :, None] + EPSILON)
    return (dense_grad, new_table, new_accum)
```

```python
import functools

import jax
import jax.numpy as jnp
import numpy as np
from jax import lax
from jax.experimental import pallas as pl
from jax.experimental.pallas import tpu as pltpu
from jax.sharding import PartitionSpec as P

LEARN_RATE = 0.1
EPSILON = 1e-08
MESH = pl.DeviceIdType.MESH
CHUNKS = 2
VMEM_LIMIT = 60 * 1024 * 1024


def pair_matrix(feature_count):
    row_index, col_index = np.tril_indices(feature_count, -1)
    pair_count = row_index.shape[0]
    matrix = np.zeros((pair_count, feature_count * feature_count), np.float32)
    matrix[np.arange(pair_count), row_index * feature_count + col_index] = 1.0
    matrix[np.arange(pair_count), col_index * feature_count + row_index] = 1.0
    return jnp.asarray(matrix)


def table_chunks(table_count):
    cut = (table_count + 1) // 2
    halves = []
    for half, (low, high) in enumerate(((0, cut), (cut, table_count))):
        edges = [low + (high - low) * k // CHUNKS for k in range(CHUNKS + 1)]
        halves.append([(half, a, b - a) for a, b in zip(edges, edges[1:]) if b > a])
    out = []
    for k in range(CHUNKS):
        for pieces in halves:
            if k < len(pieces):
                out.append(pieces[k])
    return cut, out


def neighbours():
    dp, mp = lax.axis_index("dp"), lax.axis_index("mp")
    mp_count = lax.axis_size("mp")
    across_x = (dp + 1 - 2 * (dp % 2), mp)
    across_y = (dp, (mp + mp_count // 2) % mp_count)
    core = (dp, mp + 1 - 2 * (mp % 2))
    return across_x, across_y, core


def meet(devices):
    barrier = pltpu.get_barrier_semaphore()
    for device in devices:
        pl.semaphore_signal(barrier, inc=1, device_id=device, device_id_type=MESH)
    pl.semaphore_wait(barrier, len(devices))


def gather_kernel(chunks, rows, keys, got_rows, got_keys, send, recv):
    across_x, across_y, core = neighbours()
    meet((across_x, across_y, core))

    def copies(leg, index, source_rows, source_keys, slot, device):
        _, start, length = chunks[index]
        span = pl.ds(start, length)
        return [
            pltpu.make_async_remote_copy(
                src_ref=source.at[span],
                dst_ref=target.at[slot, span],
                send_sem=send.at[leg, index, which],
                recv_sem=recv.at[leg, index, which],
                device_id=device,
                device_id_type=MESH,
            )
            for which, (source, target) in enumerate(
                ((source_rows, got_rows), (source_keys, got_keys))
            )
        ]

    outward, inward, relayed = [], [], []
    for index, (half, _, _) in enumerate(chunks):
        device = across_x if half else across_y
        outward.append(copies(1, index, rows, keys, 1, device))
        for copy in outward[-1]:
            copy.start()
    for index in range(len(chunks)):
        inward.append(copies(0, index, rows, keys, 0, core))
        for copy in inward[-1]:
            copy.start()
    for index in range(len(chunks)):
        for copy in outward[index]:
            copy.wait_recv()
        relayed.append(copies(2, index, got_rows.at[1], got_keys.at[1], 2, core))
        for copy in relayed[-1]:
            copy.start()
    for group in outward:
        for copy in group:
            copy.wait_send()
    for group in inward + relayed:
        for copy in group:
            copy.wait()


def gather(chunks, rows, keys):
    any_space = pl.BlockSpec(memory_space=pl.ANY)
    return pl.pallas_call(
        functools.partial(gather_kernel, chunks),
        out_shape=(
            jax.ShapeDtypeStruct((3,) + rows.shape, rows.dtype),
            jax.ShapeDtypeStruct((3,) + keys.shape, keys.dtype),
        ),
        in_specs=[any_space] * 2,
        out_specs=(any_space,) * 2,
        scratch_shapes=[
            pltpu.SemaphoreType.DMA((3, len(chunks), 2)),
            pltpu.SemaphoreType.DMA((3, len(chunks), 2)),
        ],
        compiler_params=pltpu.CompilerParams(collective_id=0, has_side_effects=True),
    )(rows, keys)


def sum_kernel(wanted, rows, keys, got_rows, got_keys, out):
    want = wanted[0]

    def part(key_row, row_block):
        onehot = jnp.where(want == key_row, 1.0, 0.0).astype(jnp.bfloat16)
        return jnp.dot(onehot, row_block, preferred_element_type=jnp.float32)

    total = part(keys[0], rows[0])
    for slot in range(3):
        total = total + part(got_keys[slot, 0], got_rows[slot, 0])
    out[0] = total.astype(out.dtype)


def sum_rows(cut, wanted, rows, keys, got_rows, got_keys):
    table_count, batch_rows, width = rows.shape
    targets = wanted.shape[1]
    return pl.pallas_call(
        sum_kernel,
        grid=(table_count,),
        out_shape=jax.ShapeDtypeStruct((table_count, targets, width), jnp.bfloat16),
        in_specs=[
            pl.BlockSpec((1, targets, 1), lambda t: (jnp.where(t >= cut, 1, 0), 0, 0)),
            pl.BlockSpec((1, batch_rows, width), lambda t: (t, 0, 0)),
            pl.BlockSpec((1, 1, batch_rows), lambda t: (t, 0, 0)),
            pl.BlockSpec((3, 1, batch_rows, width), lambda t: (0, t, 0, 0)),
            pl.BlockSpec((3, 1, 1, batch_rows), lambda t: (0, t, 0, 0)),
        ],
        out_specs=pl.BlockSpec((1, targets, width), lambda t: (t, 0, 0)),
    )(wanted, rows, keys, got_rows, got_keys)


def scatter_kernel(chunks, z_count, partial, out, first, mixed, last, send1, recv1, send2, recv2):
    across_x, across_y, _ = neighbours()
    dp, mp = lax.axis_index("dp"), lax.axis_index("mp")
    z = dp // 2
    my_side = (mp // 2, dp % 2)
    rows_own = out.shape[1]
    z_devices = [(((z + d) % z_count) * 2 + dp % 2, mp) for d in range(1, z_count)]
    meet([across_x, across_y] + z_devices)

    swaps = []
    for index, (half, start, length) in enumerate(chunks):
        span = pl.ds(start, length)
        other = 1 - (my_side[0] if half else my_side[1])
        swaps.append(
            pltpu.make_async_remote_copy(
                src_ref=partial.at[span, other],
                dst_ref=first.at[span],
                send_sem=send1.at[index],
                recv_sem=recv1.at[index],
                device_id=across_y if half else across_x,
                device_id_type=MESH,
            )
        )
        swaps[-1].start()
    spread = []
    for index, (half, start, length) in enumerate(chunks):
        mine = my_side[0] if half else my_side[1]
        swaps[index].wait_recv()

        def add(step, carry, start=start, mine=mine):
            t = start + step
            total = partial[t, mine].astype(jnp.float32) + first[t].astype(jnp.float32)
            total = total.astype(jnp.bfloat16)
            for owner in range(z_count):
                mixed[owner, t] = total[owner * rows_own : (owner + 1) * rows_own]
            return carry

        lax.fori_loop(0, length, add, 0)
        span = pl.ds(start, length)
        group = []
        for d in range(1, z_count):
            copy = pltpu.make_async_remote_copy(
                src_ref=mixed.at[(z + d) % z_count, span],
                dst_ref=last.at[d - 1, span],
                send_sem=send2.at[index, d - 1],
                recv_sem=recv2.at[index, d - 1],
                device_id=z_devices[d - 1],
                device_id_type=MESH,
            )
            copy.start()
            group.append(copy)
        spread.append(group)
    for index, (half, start, length) in enumerate(chunks):
        for copy in spread[index]:
            copy.wait_recv()

        def finish(step, carry, start=start):
            t = start + step
            total = mixed[z, t].astype(jnp.float32)
            for d in range(1, z_count):
                total = total + last[d - 1, t].astype(jnp.float32)
            out[t] = total
            return carry

        lax.fori_loop(0, length, finish, 0)
    for index in range(len(chunks)):
        swaps[index].wait_send()
        for copy in spread[index]:
            copy.wait_send()


def scatter(chunks, z_count, rows_own, partial):
    table_count, _, side_rows, width = partial.shape
    vmem = pl.BlockSpec(memory_space=pltpu.VMEM)
    count = len(chunks)
    return pl.pallas_call(
        functools.partial(scatter_kernel, chunks, z_count),
        out_shape=jax.ShapeDtypeStruct((table_count, rows_own, width), jnp.float32),
        in_specs=[vmem],
        out_specs=vmem,
        scratch_shapes=[
            pltpu.VMEM((table_count, side_rows, width), jnp.bfloat16),
            pltpu.VMEM((z_count, table_count, rows_own, width), jnp.bfloat16),
            pltpu.VMEM((max(1, z_count - 1), table_count, rows_own, width), jnp.bfloat16),
            pltpu.SemaphoreType.DMA((count,)),
            pltpu.SemaphoreType.DMA((count,)),
            pltpu.SemaphoreType.DMA((count, max(1, z_count - 1))),
            pltpu.SemaphoreType.DMA((count, max(1, z_count - 1))),
        ],
        compiler_params=pltpu.CompilerParams(
            collective_id=1, has_side_effects=True, vmem_limit_bytes=VMEM_LIMIT
        ),
    )(partial)


def wanted_rows(z_count, rows_own, rows_group):
    dp, mp = lax.axis_index("dp"), lax.axis_index("mp")
    side = np.arange(2)[:, None, None]
    z = np.arange(z_count)[None, :, None]
    row = np.arange(rows_own)[None, None, :]
    by_x = jnp.asarray((z * 2 + side) * rows_group + row, jnp.int32) + mp * rows_own
    by_y = (
        jnp.asarray(z * 2 * rows_group + side * 2 * rows_own + row, jnp.int32)
        + (dp % 2) * rows_group
        + (mp % 2) * rows_own
    )
    return jnp.stack([by_x.reshape(-1, 1), by_y.reshape(-1, 1)])


def per_device(sparse_vecs, dense_vec, top_cot, top_weight, owner_ids, local_rows, table, accum):
    batch_rows, table_count, row_width = sparse_vecs.shape
    feature_count = table_count + 1
    rows_own = table.shape[1]
    rows_group = lax.axis_size("mp") * rows_own
    z_count = lax.axis_size("dp") // 2
    cut, chunks = table_chunks(table_count)
    keys = (owner_ids[:, :, 0] * rows_group + local_rows).T[:, None, :]
    input_cot = jnp.einsum("bh,zh->bz", top_cot, top_weight, preferred_element_type=jnp.float32)
    symmetric = jnp.dot(
        input_cot[:, row_width:],
        pair_matrix(feature_count),
        precision=lax.Precision.HIGHEST,
        preferred_element_type=jnp.float32,
    )
    symmetric = symmetric.reshape(batch_rows, feature_count, feature_count)
    features = jnp.concatenate([dense_vec[:, None, :], sparse_vecs], axis=1).astype(jnp.float32)
    feature_grad = jnp.einsum("bij,bje->bie", symmetric, features, precision=lax.Precision.HIGHEST)
    dense_grad = (input_cot[:, :row_width] + feature_grad[:, 0]).astype(jnp.bfloat16)
    rows = feature_grad[:, 1:].astype(jnp.bfloat16).transpose(1, 0, 2)
    got_rows, got_keys = gather(chunks, rows, keys)
    wanted = wanted_rows(z_count, rows_own, rows_group)
    partial = sum_rows(cut, wanted, rows, keys, got_rows, got_keys)
    partial = partial.reshape(table_count, 2, z_count * rows_own, row_width)
    row_grad = scatter(chunks, z_count, rows_own, partial)
    new_accum = accum + jnp.mean(row_grad * row_grad, axis=-1)
    new_table = table - LEARN_RATE * row_grad / (jnp.sqrt(new_accum)[:, :, None] + EPSILON)
    return (dense_grad, new_table, new_accum)


def solution(mesh):
    in_specs = (
        P(("dp", "mp"), None, None),
        P(("dp", "mp"), None),
        P(("dp", "mp"), None),
        P(),
        P(("dp", "mp"), None, None),
        P(("dp", "mp"), None),
        P(None, ("dp", "mp"), None),
        P(None, ("dp", "mp")),
    )
    out_specs = (P(("dp", "mp"), None), P(None, ("dp", "mp"), None), P(None, ("dp", "mp")))
    return jax.shard_map(
        per_device, mesh=mesh, in_specs=in_specs, out_specs=out_specs, check_vma=False
    )
```

```python
import functools

import jax
import jax.numpy as jnp
import numpy as np
from jax import lax
from jax.experimental import pallas as pl
from jax.experimental.pallas import tpu as pltpu
from jax.sharding import PartitionSpec as P

LEARN_RATE = 0.1
EPSILON = 1e-08
MESH = pl.DeviceIdType.MESH
CHUNKS = 4
LEAD = 4
VMEM_LIMIT = 60 * 1024 * 1024


def pair_matrix(feature_count):
    row_index, col_index = np.tril_indices(feature_count, -1)
    pair_count = row_index.shape[0]
    matrix = np.zeros((pair_count, feature_count * feature_count), np.float32)
    matrix[np.arange(pair_count), row_index * feature_count + col_index] = 1.0
    matrix[np.arange(pair_count), col_index * feature_count + row_index] = 1.0
    return jnp.asarray(matrix)


def table_chunks(table_count):
    cut = (table_count + 1) // 2
    halves = []
    for half, (low, high) in enumerate(((0, cut), (cut, table_count))):
        edges = [low + (high - low) * k // CHUNKS for k in range(CHUNKS + 1)]
        halves.append([(half, a, b - a) for a, b in zip(edges, edges[1:]) if b > a])
    out = []
    for k in range(CHUNKS):
        for pieces in halves:
            if k < len(pieces):
                out.append(pieces[k])
    return cut, out


def neighbours():
    dp, mp = lax.axis_index("dp"), lax.axis_index("mp")
    mp_count = lax.axis_size("mp")
    across_x = (dp + 1 - 2 * (dp % 2), mp)
    across_y = (dp, (mp + mp_count // 2) % mp_count)
    core = (dp, mp + 1 - 2 * (mp % 2))
    return across_x, across_y, core


def meet(devices):
    barrier = pltpu.get_barrier_semaphore()
    for device in devices:
        pl.semaphore_signal(barrier, inc=1, device_id=device, device_id_type=MESH)
    pl.semaphore_wait(barrier, len(devices))


def route_kernel(
    chunks, z_count, rows, keys, out, got_rows, got_keys, partial, first, mixed, last,
    send, recv, send1, recv1, send2, recv2,
):
    across_x, across_y, core = neighbours()
    dp, mp = lax.axis_index("dp"), lax.axis_index("mp")
    z = dp // 2
    my_side = (mp // 2, dp % 2)
    rows_own = out.shape[1]
    side_rows = z_count * rows_own
    bases = (mp * 2 * side_rows, ((mp % 2) * 2 + dp % 2) * 2 * side_rows)
    z_devices = [(((z + d) % z_count) * 2 + dp % 2, mp) for d in range(1, z_count)]
    meet([across_x, across_y, core] + z_devices)
    count = len(chunks)

    def copies(leg, index, source_rows, source_keys, slot, device):
        _, start, length = chunks[index]
        span = pl.ds(start, length)
        return [
            pltpu.make_async_remote_copy(
                src_ref=source.at[span],
                dst_ref=target.at[slot, span],
                send_sem=send.at[leg, index, which],
                recv_sem=recv.at[leg, index, which],
                device_id=device,
                device_id_type=MESH,
            )
            for which, (source, target) in enumerate(
                ((source_rows, got_rows), (source_keys, got_keys))
            )
        ]

    started = []

    def begin(group):
        for copy in group:
            copy.start()
        started.extend(group)
        return group

    outward, inward, relayed, swaps, spread = [], [], [], [], []

    def send_out(index):
        if index < count:
            half = chunks[index][0]
            outward.append(
                begin(copies(1, index, rows, keys, 1, across_x if half else across_y))
            )
            inward.append(begin(copies(0, index, rows, keys, 0, core)))

    def relay(index):
        for copy in outward[index]:
            copy.wait_recv()
        relayed.append(begin(copies(2, index, got_rows.at[1], got_keys.at[1], 2, core)))

    def sums(index):
        half, start, length = chunks[index]
        for copy in inward[index] + relayed[index]:
            copy.wait_recv()
        base = bases[half]
        batch_rows = rows.shape[1]
        targets = lax.broadcasted_iota(jnp.int32, (2 * side_rows, batch_rows), 0)

        def add_table(step, carry):
            t = start + step

            def part(key_row, row_block):
                onehot = jnp.where(targets == key_row - base, 1.0, 0.0).astype(jnp.bfloat16)
                return jnp.dot(onehot, row_block, preferred_element_type=jnp.float32)

            total = part(keys[t], rows[t])
            for slot in range(3):
                total = total + part(got_keys[slot, t], got_rows[slot, t])
            total = total.astype(jnp.bfloat16)
            partial[t, 0] = total[:side_rows]
            partial[t, 1] = total[side_rows:]
            return carry

        lax.fori_loop(0, length, add_table, 0)
        span = pl.ds(start, length)
        other = 1 - (my_side[0] if half else my_side[1])
        swaps.append(
            pltpu.make_async_remote_copy(
                src_ref=partial.at[span, other],
                dst_ref=first.at[span],
                send_sem=send1.at[index],
                recv_sem=recv1.at[index],
                device_id=across_y if half else across_x,
                device_id_type=MESH,
            )
        )
        begin(swaps[-1:])

    def along_z(index):
        half, start, length = chunks[index]
        mine = my_side[0] if half else my_side[1]
        swaps[index].wait_recv()

        def add(step, carry):
            t = start + step
            total = partial[t, mine].astype(jnp.float32) + first[t].astype(jnp.float32)
            total = total.astype(jnp.bfloat16)
            for owner in range(z_count):
                mixed[owner, t] = total[owner * rows_own : (owner + 1) * rows_own]
            return carry

        lax.fori_loop(0, length, add, 0)
        span = pl.ds(start, length)
        group = [
            pltpu.make_async_remote_copy(
                src_ref=mixed.at[(z + d) % z_count, span],
                dst_ref=last.at[d - 1, span],
                send_sem=send2.at[index, d - 1],
                recv_sem=recv2.at[index, d - 1],
                device_id=z_devices[d - 1],
                device_id_type=MESH,
            )
            for d in range(1, z_count)
        ]
        spread.append(begin(group))

    def finish(index):
        _, start, length = chunks[index]
        for copy in spread[index]:
            copy.wait_recv()

        def add(step, carry):
            t = start + step
            total = mixed[z, t].astype(jnp.float32)
            for d in range(1, z_count):
                total = total + last[d - 1, t].astype(jnp.float32)
            out[t] = total
            return carry

        lax.fori_loop(0, length, add, 0)

    for index in range(LEAD):
        send_out(index)
    for index in range(count + 3):
        if index < count:
            relay(index)
            send_out(index + LEAD)
        if 0 <= index - 1 < count:
            sums(index - 1)
        if 0 <= index - 3 < count:
            along_z(index - 3)
    for index in range(count):
        finish(index)
    for copy in started:
        copy.wait_send()


def route(chunks, z_count, rows_own, rows, keys):
    table_count, batch_rows, width = rows.shape
    side_rows = z_count * rows_own
    others = max(1, z_count - 1)
    vmem = pl.BlockSpec(memory_space=pltpu.VMEM)
    count = len(chunks)
    return pl.pallas_call(
        functools.partial(route_kernel, chunks, z_count),
        out_shape=jax.ShapeDtypeStruct((table_count, rows_own, width), jnp.float32),
        in_specs=[vmem] * 2,
        out_specs=vmem,
        scratch_shapes=[
            pltpu.VMEM((3,) + rows.shape, rows.dtype),
            pltpu.VMEM((3,) + keys.shape, keys.dtype),
            pltpu.VMEM((table_count, 2, side_rows, width), jnp.bfloat16),
            pltpu.VMEM((table_count, side_rows, width), jnp.bfloat16),
            pltpu.VMEM((z_count, table_count, rows_own, width), jnp.bfloat16),
            pltpu.VMEM((others, table_count, rows_own, width), jnp.bfloat16),
            pltpu.SemaphoreType.DMA((3, count, 2)),
            pltpu.SemaphoreType.DMA((3, count, 2)),
            pltpu.SemaphoreType.DMA((count,)),
            pltpu.SemaphoreType.DMA((count,)),
            pltpu.SemaphoreType.DMA((count, others)),
            pltpu.SemaphoreType.DMA((count, others)),
        ],
        compiler_params=pltpu.CompilerParams(
            collective_id=0, has_side_effects=True, vmem_limit_bytes=VMEM_LIMIT
        ),
    )(rows, keys)


def encode_keys(cut, z_count, rows_own, owner, local):
    x, z = owner % 2, owner // 2
    mp, row = local // rows_own, local % rows_own
    y, core = mp // 2, mp % 2
    place = z * rows_own + row
    by_x = (mp * 2 + x) * (z_count * rows_own) + place
    by_y = ((core * 2 + x) * 2 + y) * (z_count * rows_own) + place
    first_half = jnp.arange(owner.shape[1])[None, :] < cut
    return jnp.where(first_half, by_x, by_y).T[:, None, :]


def per_device(sparse_vecs, dense_vec, top_cot, top_weight, owner_ids, local_rows, table, accum):
    batch_rows, table_count, row_width = sparse_vecs.shape
    feature_count = table_count + 1
    rows_own = table.shape[1]
    z_count = lax.axis_size("dp") // 2
    cut, chunks = table_chunks(table_count)
    keys = encode_keys(cut, z_count, rows_own, owner_ids[:, :, 0], local_rows)
    input_cot = jnp.einsum("bh,zh->bz", top_cot, top_weight, preferred_element_type=jnp.float32)
    symmetric = jnp.dot(
        input_cot[:, row_width:].astype(jnp.bfloat16),
        pair_matrix(feature_count).astype(jnp.bfloat16),
        preferred_element_type=jnp.bfloat16,
    )
    symmetric = symmetric.reshape(batch_rows, feature_count, feature_count)
    features = jnp.concatenate([dense_vec[:, None, :], sparse_vecs], axis=1)
    feature_grad = jnp.einsum(
        "bij,bje->bie", symmetric, features, preferred_element_type=jnp.float32
    )
    dense_grad = (input_cot[:, :row_width] + feature_grad[:, 0]).astype(jnp.bfloat16)
    rows = feature_grad[:, 1:].astype(jnp.bfloat16).transpose(1, 0, 2)
    row_grad = route(chunks, z_count, rows_own, rows, keys)
    new_accum = accum + jnp.mean(row_grad * row_grad, axis=-1)
    new_table = table - LEARN_RATE * row_grad / (jnp.sqrt(new_accum)[:, :, None] + EPSILON)
    return (dense_grad, new_table, new_accum)


def solution(mesh):
    in_specs = (
        P(("dp", "mp"), None, None),
        P(("dp", "mp"), None),
        P(("dp", "mp"), None),
        P(),
        P(("dp", "mp"), None, None),
        P(("dp", "mp"), None),
        P(None, ("dp", "mp"), None),
        P(None, ("dp", "mp")),
    )
    out_specs = (P(("dp", "mp"), None), P(None, ("dp", "mp"), None), P(None, ("dp", "mp")))
    return jax.shard_map(
        per_device, mesh=mesh, in_specs=in_specs, out_specs=out_specs, check_vma=False
    )
```

```python
import functools

import jax
import jax.numpy as jnp
import numpy as np
from jax import lax
from jax.experimental import pallas as pl
from jax.experimental.pallas import tpu as pltpu
from jax.sharding import PartitionSpec as P

LEARN_RATE = 0.1
EPSILON = 1e-08
MESH = pl.DeviceIdType.MESH
CHUNKS = 6
LEAD = 4
VMEM_LIMIT = 60 * 1024 * 1024


def pair_matrix(feature_count):
    row_index, col_index = np.tril_indices(feature_count, -1)
    pair_count = row_index.shape[0]
    matrix = np.zeros((pair_count, feature_count * feature_count), np.float32)
    matrix[np.arange(pair_count), row_index * feature_count + col_index] = 1.0
    matrix[np.arange(pair_count), col_index * feature_count + row_index] = 1.0
    return jnp.asarray(matrix)


def table_chunks(table_count):
    cut = (table_count + 1) // 2
    halves = []
    for half, (low, high) in enumerate(((0, cut), (cut, table_count))):
        edges = [low + (high - low) * k // CHUNKS for k in range(CHUNKS + 1)]
        halves.append([(half, a, b - a) for a, b in zip(edges, edges[1:]) if b > a])
    out = []
    for k in range(CHUNKS):
        for pieces in halves:
            if k < len(pieces):
                out.append(pieces[k])
    return cut, out


def neighbours():
    dp, mp = lax.axis_index("dp"), lax.axis_index("mp")
    mp_count = lax.axis_size("mp")
    across_x = (dp + 1 - 2 * (dp % 2), mp)
    across_y = (dp, (mp + mp_count // 2) % mp_count)
    core = (dp, mp + 1 - 2 * (mp % 2))
    return across_x, across_y, core


def meet(devices):
    barrier = pltpu.get_barrier_semaphore()
    for device in devices:
        pl.semaphore_signal(barrier, inc=1, device_id=device, device_id_type=MESH)
    pl.semaphore_wait(barrier, len(devices))


def route_kernel(
    chunks, z_count, rows, keys, out, got_rows, got_keys, partial, first, mixed, last,
    send, recv, send1, recv1, send2, recv2,
):
    across_x, across_y, core = neighbours()
    dp, mp = lax.axis_index("dp"), lax.axis_index("mp")
    z = dp // 2
    my_side = (mp // 2, dp % 2)
    rows_own = out.shape[1]
    side_rows = z_count * rows_own
    bases = (mp * 2 * side_rows, ((mp % 2) * 2 + dp % 2) * 2 * side_rows)
    z_devices = [(((z + d) % z_count) * 2 + dp % 2, mp) for d in range(1, z_count)]
    meet([across_x, across_y, core] + z_devices)
    count = len(chunks)

    def copies(leg, index, source_rows, source_keys, slot, device):
        _, start, length = chunks[index]
        span = pl.ds(start, length)
        return [
            pltpu.make_async_remote_copy(
                src_ref=source.at[span],
                dst_ref=target.at[slot, span],
                send_sem=send.at[leg, index, which],
                recv_sem=recv.at[leg, index, which],
                device_id=device,
                device_id_type=MESH,
            )
            for which, (source, target) in enumerate(
                ((source_rows, got_rows), (source_keys, got_keys))
            )
        ]

    started = []

    def begin(group):
        for copy in group:
            copy.start()
        started.extend(group)
        return group

    outward, inward, relayed, swaps, spread = [], [], [], [], []

    def send_out(index):
        if index < count:
            half = chunks[index][0]
            outward.append(
                begin(copies(1, index, rows, keys, 1, across_x if half else across_y))
            )
            inward.append(begin(copies(0, index, rows, keys, 0, core)))

    def relay(index):
        for copy in outward[index]:
            copy.wait_recv()
        relayed.append(begin(copies(2, index, got_rows.at[1], got_keys.at[1], 2, core)))

    def sums(index):
        half, start, length = chunks[index]
        for copy in inward[index] + relayed[index]:
            copy.wait_recv()
        base = bases[half]
        batch_rows = rows.shape[1]
        targets = lax.broadcasted_iota(jnp.int32, (2 * side_rows, batch_rows), 0)

        def add_table(step, carry):
            t = start + step

            def part(key_row, row_block):
                onehot = jnp.where(targets == key_row - base, 1.0, 0.0).astype(jnp.bfloat16)
                return jnp.dot(onehot, row_block, preferred_element_type=jnp.float32)

            total = part(keys[t], rows[t])
            for slot in range(3):
                total = total + part(got_keys[slot, t], got_rows[slot, t])
            total = total.astype(jnp.bfloat16)
            partial[t, 0] = total[:side_rows]
            partial[t, 1] = total[side_rows:]
            return carry

        lax.fori_loop(0, length, add_table, 0)
        span = pl.ds(start, length)
        other = 1 - (my_side[0] if half else my_side[1])
        swaps.append(
            pltpu.make_async_remote_copy(
                src_ref=partial.at[span, other],
                dst_ref=first.at[span],
                send_sem=send1.at[index],
                recv_sem=recv1.at[index],
                device_id=across_y if half else across_x,
                device_id_type=MESH,
            )
        )
        begin(swaps[-1:])

    def along_z(index):
        half, start, length = chunks[index]
        mine = my_side[0] if half else my_side[1]
        swaps[index].wait_recv()

        def add(step, carry):
            t = start + step
            total = partial[t, mine].astype(jnp.float32) + first[t].astype(jnp.float32)
            total = total.astype(jnp.bfloat16)
            for owner in range(z_count):
                mixed[owner, t] = total[owner * rows_own : (owner + 1) * rows_own]
            return carry

        lax.fori_loop(0, length, add, 0)
        span = pl.ds(start, length)
        group = [
            pltpu.make_async_remote_copy(
                src_ref=mixed.at[(z + d) % z_count, span],
                dst_ref=last.at[d - 1, span],
                send_sem=send2.at[index, d - 1],
                recv_sem=recv2.at[index, d - 1],
                device_id=z_devices[d - 1],
                device_id_type=MESH,
            )
            for d in range(1, z_count)
        ]
        spread.append(begin(group))

    def finish(index):
        _, start, length = chunks[index]
        for copy in spread[index]:
            copy.wait_recv()

        def add(step, carry):
            t = start + step
            total = mixed[z, t].astype(jnp.float32)
            for d in range(1, z_count):
                total = total + last[d - 1, t].astype(jnp.float32)
            out[t] = total
            return carry

        lax.fori_loop(0, length, add, 0)

    for index in range(LEAD):
        send_out(index)
    for index in range(count + 3):
        if index < count:
            relay(index)
            send_out(index + LEAD)
        if 0 <= index - 1 < count:
            sums(index - 1)
        if 0 <= index - 3 < count:
            along_z(index - 3)
    for index in range(count):
        finish(index)
    for copy in started:
        copy.wait_send()


def route(chunks, z_count, rows_own, rows, keys):
    table_count, batch_rows, width = rows.shape
    side_rows = z_count * rows_own
    others = max(1, z_count - 1)
    vmem = pl.BlockSpec(memory_space=pltpu.VMEM)
    count = len(chunks)
    return pl.pallas_call(
        functools.partial(route_kernel, chunks, z_count),
        out_shape=jax.ShapeDtypeStruct((table_count, rows_own, width), jnp.float32),
        in_specs=[vmem] * 2,
        out_specs=vmem,
        scratch_shapes=[
            pltpu.VMEM((3,) + rows.shape, rows.dtype),
            pltpu.VMEM((3,) + keys.shape, keys.dtype),
            pltpu.VMEM((table_count, 2, side_rows, width), jnp.bfloat16),
            pltpu.VMEM((table_count, side_rows, width), jnp.bfloat16),
            pltpu.VMEM((z_count, table_count, rows_own, width), jnp.bfloat16),
            pltpu.VMEM((others, table_count, rows_own, width), jnp.bfloat16),
            pltpu.SemaphoreType.DMA((3, count, 2)),
            pltpu.SemaphoreType.DMA((3, count, 2)),
            pltpu.SemaphoreType.DMA((count,)),
            pltpu.SemaphoreType.DMA((count,)),
            pltpu.SemaphoreType.DMA((count, others)),
            pltpu.SemaphoreType.DMA((count, others)),
        ],
        compiler_params=pltpu.CompilerParams(
            collective_id=0, has_side_effects=True, vmem_limit_bytes=VMEM_LIMIT
        ),
    )(rows, keys)


def encode_keys(cut, z_count, rows_own, owner, local):
    x, z = owner % 2, owner // 2
    mp, row = local // rows_own, local % rows_own
    y, core = mp // 2, mp % 2
    place = z * rows_own + row
    by_x = (mp * 2 + x) * (z_count * rows_own) + place
    by_y = ((core * 2 + x) * 2 + y) * (z_count * rows_own) + place
    first_half = jnp.arange(owner.shape[1])[None, :] < cut
    return jnp.where(first_half, by_x, by_y).T[:, None, :]


def per_device(sparse_vecs, dense_vec, top_cot, top_weight, owner_ids, local_rows, table, accum):
    batch_rows, table_count, row_width = sparse_vecs.shape
    feature_count = table_count + 1
    rows_own = table.shape[1]
    z_count = lax.axis_size("dp") // 2
    cut, chunks = table_chunks(table_count)
    keys = encode_keys(cut, z_count, rows_own, owner_ids[:, :, 0], local_rows)
    input_cot = jnp.einsum("bh,zh->bz", top_cot, top_weight, preferred_element_type=jnp.float32)
    symmetric = jnp.dot(
        input_cot[:, row_width:].astype(jnp.bfloat16),
        pair_matrix(feature_count).astype(jnp.bfloat16),
        preferred_element_type=jnp.bfloat16,
    )
    symmetric = symmetric.reshape(batch_rows, feature_count, feature_count)
    features = jnp.concatenate([dense_vec[:, None, :], sparse_vecs], axis=1)
    feature_grad = jnp.einsum(
        "bij,bje->bie", symmetric, features, preferred_element_type=jnp.float32
    )
    dense_grad = (input_cot[:, :row_width] + feature_grad[:, 0]).astype(jnp.bfloat16)
    rows = feature_grad[:, 1:].astype(jnp.bfloat16).transpose(1, 0, 2)
    row_grad = route(chunks, z_count, rows_own, rows, keys)
    new_accum = accum + jnp.mean(row_grad * row_grad, axis=-1)
    new_table = table - LEARN_RATE * row_grad / (jnp.sqrt(new_accum)[:, :, None] + EPSILON)
    return (dense_grad, new_table, new_accum)


def solution(mesh):
    in_specs = (
        P(("dp", "mp"), None, None),
        P(("dp", "mp"), None),
        P(("dp", "mp"), None),
        P(),
        P(("dp", "mp"), None, None),
        P(("dp", "mp"), None),
        P(None, ("dp", "mp"), None),
        P(None, ("dp", "mp")),
    )
    out_specs = (P(("dp", "mp"), None), P(None, ("dp", "mp"), None), P(None, ("dp", "mp")))
    return jax.shard_map(
        per_device, mesh=mesh, in_specs=in_specs, out_specs=out_specs, check_vma=False
    )
```
